32 devices in a mesh: tok: 16 (over z, y, x), head: 2 (over core).
Axes of the slice: x: 2, y: 2, z: 4, core: 2. Of those that a mesh axis runs over, the one named last changes fastest.
Arguments:
- query_rows: bfloat16 [6144, 2048], P('tok', 'head'), may hold values from -6 to 6
- key_rows: bfloat16 [6144, 1024], P('tok', 'head'), may hold values from -6 to 6
- value_rows: bfloat16 [6144, 1024], P('tok', 'head'), may hold values from -6 to 6
- out_grad: bfloat16 [6144, 2048], P('tok', 'head'), may hold values from -96 to 96
- log_norm: float32 [6144, 16], P('tok', 'head'), may hold values from 6.5 to 8
- delta_rows: float32 [6144, 16], P('tok', 'head'), may hold values from -48 to 48
- window_len: int32 [16], P('head'), may hold values from 896 to 1024, as said below
- activations: bfloat16 [6144, 5376], P('tok'), may hold values from -6 to 6
- value_weight: bfloat16 [5376, 1024], P('tok', 'head')
- row_state: float32 [2, 5376], P('head', 'tok'), as said below
- col_state: float32 [16, 1024], P('tok', 'head'), as said below
Outputs:
- query_grad: bfloat16 [6144, 2048], P('tok', 'head')
- key_grad: bfloat16 [6144, 1024], P('tok', 'head')
- value_grad: bfloat16 [6144, 1024], P('tok', 'head')
- new_weight: bfloat16 [5376, 1024], P('tok', 'head')
- update_dir: float32 [5376, 1024], P('tok', 'head')
The draws below stay inside these ranges and needn't reach their ends.
Inputs may be any that keep to these rules, and one draw needn't show every extreme that they name: `window_len`: every head's window is one of the integers from 896 to 1024, and some head has exactly 1024. `row_state`: positive. `col_state`: positive.
All inputs are finite; a program needn't handle non-finite values.
Results may differ from the reference program's by a relative error of at most 0.005.
Values may be sent and summed in bfloat16 or wider, within the bound.
A program may use at most 128 MiB of HBM per device.

```python
import jax
import jax.numpy as jnp
from jax import lax

D = 5376
HD = 128
Q_HEADS = 16
KV_HEADS = 8
WINDOW = 1024
TOK_DEV = 384
GROUP = 2
QD = 2048
KVD = 1024
SPAN = 1408
TOKENS = 6144
N_TOK = 16
N_HEAD = 2


def draw_window_len(key, part):
    shorter = jax.random.randint(key, (Q_HEADS,), 0, WINDOW // 8 + 1)
    picked = jax.random.randint(jax.random.fold_in(key, 7), (), 0, Q_HEADS)
    shorter = jnp.where(jnp.arange(Q_HEADS) == picked, 0, shorter)
    return (WINDOW - shorter).astype(jnp.int32)


def draw_row_state(key, part):
    spread = jax.random.uniform(key, (N_HEAD, D), jnp.float32, 0.0, 1.0)
    return TOKENS * 0.2 * 10.0 ** spread


def draw_col_state(key, part):
    shard = jnp.arange(N_TOK, dtype=jnp.float32)[:, None] / max(N_TOK - 1, 1)
    jitter = jax.random.uniform(key, (N_TOK, KVD), jnp.float32, -0.3, 0.3)
    power = 1.5 - 3.0 * shard + jitter
    return TOKENS * 0.64 * 10.0 ** power


def draw_value_weight(key, part):
    key_base = jax.random.fold_in(key, 11)
    key_rows = jax.random.fold_in(key, 12)
    key_cols = jax.random.fold_in(key, 13)
    base = jnp.clip(jax.random.normal(key_base, (D, KVD), jnp.float32), -4.0, 4.0)
    row_pos = jnp.arange(D, dtype=jnp.float32) / D
    row_jitter = jax.random.uniform(key_rows, (D,), jnp.float32, 0.7, 1.4)
    col_scale = 10.0 ** jax.random.uniform(key_cols, (KVD,), jnp.float32, 0.0, 1.0)
    row_scale = 10.0 ** row_pos * row_jitter
    return (base * row_scale[:, None] * col_scale[None, :] / jnp.sqrt(jnp.float32(D))).astype(jnp.bfloat16)


def raised(drawn, stream_key, source, target, blocks, factor):
    owner, partner = [(jnp.arange(drawn.shape[position]) // (drawn.shape[position] // blocks)).reshape([-1 if axis == position else 1 for axis in range(drawn.ndim)]) for position in (source, target)]
    chosen = jax.random.permutation(stream_key, blocks)[partner]
    strong = (owner == chosen) | (owner == (partner + blocks // 2) % blocks)
    return jnp.where(strong, factor * drawn, drawn)


def block_scale(stream_key, extent, shards, least, largest):
    factor_of, own = 1.0, jax.random.fold_in(stream_key, 6)
    for dim, parts in shards:
        draws = jnp.exp(jax.random.uniform(jax.random.fold_in(own, dim), (parts,), jnp.float32, least / len(shards), largest / len(shards)))
        factor_of = factor_of * jnp.repeat(draws, extent[dim] // parts).reshape([-1 if axis == dim else 1 for axis in range(len(extent))])
    return factor_of


def centred(stream_key, extent, scale, most, pieces=(), kind=jnp.bfloat16):
    entries = scale * jax.random.normal(stream_key, extent, jnp.float32)
    if pieces:
        entries = entries * block_scale(stream_key, extent, pieces, -0.22, 0.18)
    return jnp.clip(entries, -most, most).astype(kind)


def bell_draw_with(key, shape, scale, most, pieces, heavy, held_as=jnp.bfloat16):
    entries = scale * jax.random.normal(key, shape, jnp.float32)
    if pieces:
        entries = entries * block_scale(key, shape, pieces, -0.22, 0.18)
    return jnp.clip(raised(entries, jax.random.fold_in(key, 3), *heavy), -most, most).astype(held_as)


def setup_inputs(seed: int = 0) -> dict:
    seeds = jax.random.split(jax.random.key(seed), 12)
    return {
        "query_rows": centred(seeds[0], (TOKENS, QD), 1.0, 6.0, ((0, 16), (1, 2))),
        "key_rows": centred(seeds[1], (TOKENS, KVD), 1.0, 6.0, ((0, 16), (1, 2))),
        "value_rows": centred(seeds[2], (TOKENS, KVD), 1.0, 6.0, ((0, 16), (1, 2))),
        "out_grad": centred(seeds[3], (TOKENS, QD), 16.0, 96.0, ((0, 16), (1, 2))),
        "log_norm": jnp.clip(6.5 + 1.5 * jax.random.uniform(seeds[4], (TOKENS, Q_HEADS), jnp.float32) ** block_scale(seeds[4], (TOKENS, Q_HEADS), ((0, 16), (1, 2)), -0.2, 0.2), 6.5, 8.0),
        "delta_rows": centred(seeds[5], (TOKENS, Q_HEADS), 8.0, 48.0, ((0, 16), (1, 2)), jnp.float32),
        "window_len": draw_window_len(jax.random.fold_in(seeds[11], 71), 0),
        "activations": bell_draw_with(seeds[7], (TOKENS, D), 1.0, 6.0, ((0, 16),), (0, 1, 16, 2.0)),
        "value_weight": draw_value_weight(jax.random.fold_in(seeds[11], 71), 0),
        "row_state": draw_row_state(jax.random.fold_in(seeds[11], 71), 0),
        "col_state": draw_col_state(jax.random.fold_in(seeds[11], 71), 0),
    }


QUERY_SCALE = 1.0 / 12.0
DECAY_RATE = 0.9
LEARN_RATE = 0.05

def attend_block(query_blk, key_blk, value_blk, grad_blk, norm_blk, delta_blk, window_len, first_query, first_key):
    query_f = query_blk.astype(jnp.float32)
    key_f = key_blk.astype(jnp.float32)
    value_f = value_blk.astype(jnp.float32)
    grad_f = grad_blk.astype(jnp.float32)
    scores = jnp.einsum('tkgd,skd->kgts', query_f, key_f) * QUERY_SCALE
    query_pos = first_query + jnp.arange(TOK_DEV, dtype=jnp.int32)
    key_pos = first_key + jnp.arange(SPAN, dtype=jnp.int32)
    distance = query_pos[:, None] - key_pos[None, :]
    limits = window_len.reshape(KV_HEADS, GROUP)[:, :, None, None]
    visible = (distance[None, None] >= 0) & (distance[None, None] < limits) & (key_pos >= 0)[None, None, None, :]
    norm_t = jnp.transpose(norm_blk.reshape(TOK_DEV, KV_HEADS, GROUP), (1, 2, 0))
    delta_t = jnp.transpose(delta_blk.reshape(TOK_DEV, KV_HEADS, GROUP), (1, 2, 0))
    prob_full = jnp.where(visible, jnp.exp(scores - norm_t[..., None]), 0.0)
    prob_low = lax.optimization_barrier(prob_full.astype(jnp.bfloat16)).astype(jnp.float32)
    value_part = jnp.einsum('kgts,tkgd->skd', prob_low, grad_f)
    prob_grad = jnp.einsum('tkgd,skd->kgts', grad_f, value_f)
    score_grad = QUERY_SCALE * prob_full * (prob_grad - delta_t[..., None])
    score_grad = lax.optimization_barrier(score_grad.astype(jnp.bfloat16)).astype(jnp.float32)
    query_part = jnp.einsum('kgts,skd->tkgd', score_grad, key_f)
    key_part = jnp.einsum('kgts,tkgd->skd', score_grad, query_f)
    return (query_part, key_part, value_part)

def reference(query_rows, key_rows, value_rows, out_grad, log_norm, delta_rows, window_len, activations, value_weight, row_state, col_state):
    pad_rows = WINDOW
    query4 = query_rows.reshape(TOKENS, KV_HEADS, GROUP, HD)
    grad4 = out_grad.reshape(TOKENS, KV_HEADS, GROUP, HD)
    key_pad = jnp.concatenate([jnp.zeros((pad_rows, KVD), jnp.bfloat16), key_rows], axis=0).reshape(pad_rows + TOKENS, KV_HEADS, HD)
    value_pad = jnp.concatenate([jnp.zeros((pad_rows, KVD), jnp.bfloat16), value_rows], axis=0).reshape(pad_rows + TOKENS, KV_HEADS, HD)
    zeros_acc = jnp.zeros((pad_rows + TOKENS, KV_HEADS, HD), jnp.float32)

    def step_block(carry, index):
        key_acc, value_acc = carry
        start = (index * TOK_DEV).astype(jnp.int32)
        query_blk = lax.dynamic_slice_in_dim(query4, start, TOK_DEV, 0)
        grad_blk = lax.dynamic_slice_in_dim(grad4, start, TOK_DEV, 0)
        norm_blk = lax.dynamic_slice_in_dim(log_norm, start, TOK_DEV, 0)
        delta_blk = lax.dynamic_slice_in_dim(delta_rows, start, TOK_DEV, 0)
        key_blk = lax.dynamic_slice_in_dim(key_pad, start, SPAN, 0)
        value_blk = lax.dynamic_slice_in_dim(value_pad, start, SPAN, 0)
        query_part, key_part, value_part = attend_block(query_blk, key_blk, value_blk, grad_blk, norm_blk, delta_blk, window_len, start, start - pad_rows)
        key_acc = lax.dynamic_update_slice_in_dim(key_acc, lax.dynamic_slice_in_dim(key_acc, start, SPAN, 0) + key_part, start, 0)
        value_acc = lax.dynamic_update_slice_in_dim(value_acc, lax.dynamic_slice_in_dim(value_acc, start, SPAN, 0) + value_part, start, 0)
        return ((key_acc, value_acc), query_part)
    (key_acc, value_acc), query_parts = lax.scan(step_block, (zeros_acc, zeros_acc), jnp.arange(N_TOK, dtype=jnp.int32))
    query_grad = query_parts.reshape(TOKENS, QD).astype(jnp.bfloat16)
    key_grad = key_acc[pad_rows:].reshape(TOKENS, KVD).astype(jnp.bfloat16)
    value_grad = value_acc[pad_rows:].reshape(TOKENS, KVD).astype(jnp.bfloat16)
    weight_grad = lax.dot_general(activations, value_grad, (((0,), (0,)), ((), ())), preferred_element_type=jnp.float32)
    row_blk = D // N_TOK
    col_blk = KVD // N_HEAD
    blocks = weight_grad.reshape(N_TOK, row_blk, N_HEAD, col_blk)
    squares = blocks * blocks
    row_new = lax.optimization_barrier(jnp.mean(squares, axis=3))
    col_new = lax.optimization_barrier(jnp.mean(squares, axis=1))
    row_old = jnp.transpose(row_state.reshape(N_HEAD, N_TOK, row_blk), (1, 2, 0))
    col_old = col_state.reshape(N_TOK, N_HEAD, col_blk)
    row_mix = DECAY_RATE * row_old + (1.0 - DECAY_RATE) * row_new
    col_mix = DECAY_RATE * col_old + (1.0 - DECAY_RATE) * col_new
    row_mean = lax.optimization_barrier(jnp.mean(row_mix, axis=1))
    second = row_mix[:, :, :, None] * col_mix[:, None, :, :] / row_mean[:, None, :, None]
    scaled = blocks / jnp.sqrt(second)
    weight_f = value_weight.astype(jnp.float32)
    rms_scaled = jnp.sqrt(jnp.sum(scaled * scaled) / (D * KVD))
    rms_weight = jnp.sqrt(jnp.sum(weight_f * weight_f) / (D * KVD))
    update_dir = (rms_weight * scaled / jnp.maximum(1.0, rms_scaled)).reshape(D, KVD)
    new_weight = (weight_f - LEARN_RATE * update_dir).astype(jnp.bfloat16)
    return (query_grad, key_grad, value_grad, new_weight, update_dir)
```

```python
import functools
import math

import jax
import jax.numpy as jnp
from jax import lax
from jax.experimental import pallas as pl
from jax.experimental.pallas import tpu as pltpu
from jax.sharding import PartitionSpec as P

HD = 128
WINDOW = 1024
QUERY_SCALE = 1.0 / 12.0
DECAY_RATE = 0.9
LEARN_RATE = 0.05
F32 = jnp.float32
BF16 = jnp.bfloat16
MESH = pl.DeviceIdType.MESH


def passed_along(x, axis, by):
    count = lax.axis_size(axis)
    pairs = [(i, i + by) for i in range(count) if 0 <= i + by < count]
    return lax.ppermute(x, axis, pairs)


def prob_t(keys, query, norm_row, limit, first_key, position):
    scores = (
        lax.dot_general(keys, query, (((1,), (1,)), ((), ())), preferred_element_type=F32)
        * QUERY_SCALE
    )
    key_index = first_key + lax.broadcasted_iota(jnp.int32, scores.shape, 0)
    distance = WINDOW + lax.broadcasted_iota(jnp.int32, scores.shape, 1) - key_index
    visible = (distance >= 0) & (distance < limit) & (key_index >= WINDOW - position)
    return jnp.where(visible, jnp.exp(scores - norm_row), 0.0)


def value_kernel(first_key, group, limit_ref, pos_ref, q_ref, g_ref, n_ref, k_ref, o_ref):
    kv = pl.program_id(0)
    total = None
    for member in range(group):
        cols = slice(member * HD, (member + 1) * HD)
        prob = prob_t(
            k_ref[...], q_ref[:, cols], n_ref[0, member : member + 1, :],
            limit_ref[kv * group + member], first_key, pos_ref[0],
        )
        part = jnp.dot(prob.astype(BF16), g_ref[:, cols], preferred_element_type=F32)
        total = part if total is None else total + part
    o_ref[...] = total.astype(o_ref.dtype)


def value_part(first_key, group, out_type, limits, pos, query, grad, norm_t, keys):
    tok_len, rows = query.shape[0], keys.shape[0]
    kv_local = keys.shape[1] // HD
    smem = pl.BlockSpec(memory_space=pltpu.SMEM)
    wide = pl.BlockSpec((tok_len, group * HD), lambda i: (0, i))
    return pl.pallas_call(
        functools.partial(value_kernel, first_key, group),
        grid=(kv_local,),
        out_shape=jax.ShapeDtypeStruct((rows, kv_local * HD), out_type),
        in_specs=[
            smem, smem, wide, wide,
            pl.BlockSpec((1, group, tok_len), lambda i: (i, 0, 0)),
            pl.BlockSpec((rows, HD), lambda i: (0, i)),
        ],
        out_specs=pl.BlockSpec((rows, HD), lambda i: (0, i)),
        cost_estimate=pl.CostEstimate(
            flops=3_000_000_000, bytes_accessed=4_000_000, transcendentals=0
        ),
        name=f"value_part_{first_key}",
    )(limits, pos, query, grad, norm_t, keys)


def score_kernel(firsts, group, limit_ref, pos_ref, q_ref, g_ref, n_ref, d_ref, *refs):
    count = len(firsts)
    k_refs, v_refs = refs[:count], refs[count : 2 * count]
    dq_ref, dk_refs = refs[2 * count], refs[2 * count + 1 :]
    kv = pl.program_id(0)
    queries = [None] * group
    for piece, first_key in enumerate(firsts):
        keys, values = k_refs[piece][...], v_refs[piece][...]
        key_total = None
        for member in range(group):
            cols = slice(member * HD, (member + 1) * HD)
            query = q_ref[:, cols]
            prob = prob_t(
                keys, query, n_ref[0, member : member + 1, :],
                limit_ref[kv * group + member], first_key, pos_ref[0],
            )
            dprob = lax.dot_general(
                values, g_ref[:, cols], (((1,), (1,)), ((), ())), preferred_element_type=F32
            )
            dscore = (
                QUERY_SCALE * prob * (dprob - d_ref[0, member : member + 1, :])
            ).astype(BF16)
            part = jnp.dot(dscore, query, preferred_element_type=F32)
            key_total = part if key_total is None else key_total + part
            part = lax.dot_general(
                dscore, keys, (((0,), (0,)), ((), ())), preferred_element_type=F32
            )
            queries[member] = part if queries[member] is None else queries[member] + part
        dk_refs[piece][...] = key_total.astype(dk_refs[piece].dtype)
    for member in range(group):
        dq_ref[:, member * HD : (member + 1) * HD] = queries[member].astype(dq_ref.dtype)


def score_part(firsts, group, types, limits, pos, query, grad, norm_t, delta_t, keys, values):
    tok_len = query.shape[0]
    kv_local = keys[0].shape[1] // HD
    smem = pl.BlockSpec(memory_space=pltpu.SMEM)
    wide = pl.BlockSpec((tok_len, group * HD), lambda i: (0, i))
    rows_t = pl.BlockSpec((1, group, tok_len), lambda i: (i, 0, 0))
    narrow = [pl.BlockSpec((k.shape[0], HD), lambda i: (0, i)) for k in keys]
    return pl.pallas_call(
        functools.partial(score_kernel, firsts, group),
        grid=(kv_local,),
        out_shape=[jax.ShapeDtypeStruct(query.shape, BF16)]
        + [jax.ShapeDtypeStruct(k.shape, t) for k, t in zip(keys, types)],
        in_specs=[smem, smem, wide, wide, rows_t, rows_t] + narrow + narrow,
        out_specs=[wide] + narrow,
        cost_estimate=pl.CostEstimate(
            flops=20_000_000_000, bytes_accessed=8_000_000, transcendentals=0
        ),
        name="score_part",
    )(limits, pos, query, grad, norm_t, delta_t, *keys, *values)


def bit_orders(bits, streams):
    heads = [(0, 1, 2), (1, 0, 2), (2, 0, 1), (1, 2, 0)] if bits >= 3 else [tuple(range(bits))]
    orders = []
    for s in range(streams):
        head = heads[s % len(heads)]
        orders.append(tuple(head) + tuple(range(len(head), bits)))
    return orders


def weight_kernel(
    n, n_head, streams,
    a_ref, v_ref, w_ref, rs_ref, cs_ref, upd_ref, new_ref,
    acc, sbuf, rbuf, xs, xr, scaled_ref, s_sem, r_sem, xs_sem, xr_sem,
):
    bits, head_bits = int(math.log2(n)), int(math.log2(n_head))
    me, hd = lax.axis_index("tok"), lax.axis_index("head")
    width = acc.shape[-1]
    rows = acc.shape[2]
    orders = bit_orders(bits, streams)

    def bit_of(index, k):
        return lax.rem(index // (1 << k), 2)

    def flipped(index, k):
        return index + (1 << k) * (1 - 2 * bit_of(index, k))

    partners = [{"tok": flipped(me, k)} for k in range(bits)]
    partners += [{"head": flipped(hd, k)} for k in range(head_bits)]
    barrier = pltpu.get_barrier_semaphore()
    for partner in partners:
        pl.semaphore_signal(barrier, inc=1, device_id=partner, device_id_type=MESH)

    def block_at(order, phase, j, other):
        index = 0
        for k in order[:phase]:
            index = index + (1 << k) * bit_of(me, k)
        mine = bit_of(me, order[phase])
        index = index + (1 << order[phase]) * ((1 - mine) if other else mine)
        for i, k in enumerate(sorted(order[phase + 1 :])):
            index = index + (1 << k) * lax.rem(j // (1 << i), 2)
        return index

    counts = [n >> (p + 1) for p in range(bits)]
    starts = [sum(counts[:p]) for p in range(bits)]

    def copy_of(s, p):
        here = pl.ds(starts[p], counts[p])
        return pltpu.make_async_remote_copy(
            src_ref=sbuf.at[s, here],
            dst_ref=rbuf.at[s, here],
            send_sem=s_sem.at[s, p],
            recv_sem=r_sem.at[s, p],
            device_id=partners[orders[s][p]],
            device_id_type=MESH,
        )

    def product(s, block):
        return jnp.dot(
            a_ref[block], v_ref[:, s * width : (s + 1) * width], preferred_element_type=F32
        )

    for s in range(streams):
        @pl.loop(0, counts[0])
        def _(j, s=s):
            sbuf[s, j] = product(s, block_at(orders[s], 0, j, True)).astype(BF16)

        if s == 0:
            pl.semaphore_wait(barrier, len(partners))
        copy_of(s, 0).start()
    for s in range(streams):
        @pl.loop(0, counts[0])
        def _(j, s=s):
            block = block_at(orders[s], 0, j, False)
            acc[s, block] = product(s, block)

    weight_f = w_ref[...].astype(F32)
    weight_sum = jnp.sum(weight_f * weight_f)

    for p in range(bits):
        for s in range(streams):
            copy_of(s, p).wait_recv()

            @pl.loop(0, counts[p])
            def _(j, s=s, p=p):
                block = block_at(orders[s], p, j, False)
                acc[s, block] = acc[s, block] + rbuf[s, starts[p] + j].astype(F32)

            if p + 1 < bits:
                @pl.loop(0, counts[p + 1])
                def _(j, s=s, p=p):
                    block = block_at(orders[s], p + 1, j, True)
                    sbuf[s, starts[p + 1] + j] = acc[s, block].astype(BF16)

                copy_of(s, p + 1).start()

    total_width = width * streams
    row_sum = jnp.zeros((rows, 1), F32)
    for s in range(streams):
        wg = acc[s, me]
        row_sum = row_sum + jnp.sum(wg * wg, axis=1, keepdims=True)
    row_mix = DECAY_RATE * rs_ref[...] + (1.0 - DECAY_RATE) * (row_sum / total_width)
    row_mean = jnp.sum(row_mix) / rows
    scaled_sum = jnp.float32(0.0)
    for s in range(streams):
        wg = acc[s, me]
        cols = slice(s * width, (s + 1) * width)
        col_new = jnp.sum(wg * wg, axis=0, keepdims=True) / rows
        col_mix = DECAY_RATE * cs_ref[:, cols] + (1.0 - DECAY_RATE) * col_new
        scaled = wg / jnp.sqrt(row_mix * col_mix / row_mean)
        scaled_ref[:, cols] = scaled
        scaled_sum = scaled_sum + jnp.sum(scaled * scaled)

    xs[0, :8] = jnp.full((8, 128), scaled_sum, F32)
    xs[0, 8:] = jnp.full((8, 128), weight_sum, F32)
    for i, partner in enumerate(partners):
        copy = pltpu.make_async_remote_copy(
            src_ref=xs.at[i], dst_ref=xr.at[i],
            send_sem=xs_sem.at[i], recv_sem=xr_sem.at[i],
            device_id=partner, device_id_type=MESH,
        )
        copy.start()
        copy.wait()
        xs[i + 1] = xs[i] + xr[i]
    sums = xs[len(partners)]
    size = float(rows * n * total_width * n_head)
    rms_scaled = jnp.sqrt(sums[0:1, 0:1] / size)
    rms_weight = jnp.sqrt(sums[8:9, 0:1] / size)
    update = rms_weight * scaled_ref[...] / jnp.maximum(1.0, rms_scaled)
    upd_ref[...] = update
    new_ref[...] = (w_ref[...].astype(F32) - LEARN_RATE * update).astype(BF16)
    for p in range(bits):
        for s in range(streams):
            copy_of(s, p).wait_send()


def weight_update(n, n_head, act_t, value_grad, weight, row_state, col_state):
    rows, width = act_t.shape[1], value_grad.shape[1]
    streams = 4 if width % 512 == 0 else 1
    part = width // streams
    bits, head_bits = int(math.log2(n)), int(math.log2(n_head))
    steps = bits + head_bits
    vmem = pl.BlockSpec(memory_space=pltpu.VMEM)
    return pl.pallas_call(
        functools.partial(weight_kernel, n, n_head, streams),
        out_shape=[
            jax.ShapeDtypeStruct((rows, width), F32),
            jax.ShapeDtypeStruct((rows, width), BF16),
        ],
        in_specs=[vmem] * 5,
        out_specs=[vmem] * 2,
        scratch_shapes=[
            pltpu.VMEM((streams, n, rows, part), F32),
            pltpu.VMEM((streams, n - 1, rows, part), BF16),
            pltpu.VMEM((streams, n - 1, rows, part), BF16),
            pltpu.VMEM((steps + 1, 16, 128), F32),
            pltpu.VMEM((steps, 16, 128), F32),
            pltpu.VMEM((rows, width), F32),
            pltpu.SemaphoreType.DMA((streams, bits)),
            pltpu.SemaphoreType.DMA((streams, bits)),
            pltpu.SemaphoreType.DMA((steps,)),
            pltpu.SemaphoreType.DMA((steps,)),
        ],
        compiler_params=pltpu.CompilerParams(
            collective_id=0, has_side_effects=True, vmem_limit_bytes=56 * 1024 * 1024
        ),
        cost_estimate=pl.CostEstimate(
            flops=60_000_000_000, bytes_accessed=8_000_000, transcendentals=0
        ),
        name="weight_update",
    )(act_t, value_grad, weight, row_state, col_state)


def shards(
    query_rows, key_rows, value_rows, out_grad, log_norm, delta_rows, window_len,
    activations, value_weight, row_state, col_state, *, n, n_head,
):
    tok_len = query_rows.shape[0]
    kv_local = key_rows.shape[1] // HD
    group = query_rows.shape[1] // key_rows.shape[1]
    reach = (WINDOW + tok_len - 1) // tok_len
    offsets = list(range(1, reach + 1))
    pos = (lax.axis_index("tok") * tok_len).astype(jnp.int32).reshape(1)
    norm_t = log_norm.T.reshape(kv_local, group, tok_len)
    delta_t = delta_rows.T.reshape(kv_local, group, tok_len)
    act_t = activations.T.reshape(n, activations.shape[1] // n, tok_len)

    def sent_rows(offset):
        return min(tok_len, WINDOW - (offset - 1) * tok_len)

    def first_of(offset):
        return max(0, WINDOW - offset * tok_len)

    far_keys = [passed_along(key_rows[tok_len - sent_rows(o) :], "tok", o) for o in offsets]
    far_values = [passed_along(value_rows[tok_len - sent_rows(o) :], "tok", o) for o in offsets]

    def value_of(first_key, out_type, keys):
        return value_part(
            first_key, group, out_type, window_len, pos, query_rows, out_grad, norm_t, keys
        )

    def gathered(own, far):
        total = own
        for o, piece in zip(offsets, far):
            arrived = passed_along(piece, "tok", -o).astype(F32)
            total = total + jnp.pad(arrived, ((tok_len - arrived.shape[0], 0), (0, 0)))
        return total.astype(BF16)

    value_own = value_of(WINDOW, F32, key_rows)
    value_far = [value_of(first_of(o), BF16, k) for o, k in zip(offsets, far_keys)]
    value_grad = gathered(value_own, value_far)
    firsts = tuple([WINDOW] + [first_of(o) for o in offsets])
    query_grad, key_own, *key_far = score_part(
        firsts, group, [F32] + [BF16] * reach, window_len, pos, query_rows, out_grad,
        norm_t, delta_t, [key_rows] + far_keys, [value_rows] + far_values,
    )
    key_grad = gathered(key_own, key_far)
    update_dir, new_weight = weight_update(
        n, n_head, act_t, value_grad, value_weight, row_state.reshape(-1, 1), col_state
    )
    return (query_grad, key_grad, value_grad, new_weight, update_dir)


def solution(mesh):
    both = P("tok", "head")
    return jax.shard_map(
        functools.partial(shards, n=mesh.shape["tok"], n_head=mesh.shape["head"]),
        mesh=mesh,
        in_specs=(
            both, both, both, both, both, both, P("head"), P("tok", None),
            both, P("head", "tok"), both,
        ),
        out_specs=(both,) * 5,
        check_vma=False,
    )
```

```python
import functools
import math

import jax
import jax.numpy as jnp
from jax import lax
from jax.experimental import pallas as pl
from jax.experimental.pallas import tpu as pltpu
from jax.sharding import PartitionSpec as P

HD = 128
WINDOW = 1024
QUERY_SCALE = 1.0 / 12.0
DECAY_RATE = 0.9
LEARN_RATE = 0.05
F32 = jnp.float32
BF16 = jnp.bfloat16
MESH = pl.DeviceIdType.MESH


def passed_along(x, axis, by):
    count = lax.axis_size(axis)
    pairs = [(i, i + by) for i in range(count) if 0 <= i + by < count]
    return lax.ppermute(x, axis, pairs)


def prob_t(keys, query, norm_row, limit, first_key, position):
    scores = (
        lax.dot_general(keys, query, (((1,), (1,)), ((), ())), preferred_element_type=F32)
        * QUERY_SCALE
    )
    key_index = first_key + lax.broadcasted_iota(jnp.int32, scores.shape, 0)
    distance = WINDOW + lax.broadcasted_iota(jnp.int32, scores.shape, 1) - key_index
    visible = (distance >= 0) & (distance < limit) & (key_index >= WINDOW - position)
    return jnp.where(visible, jnp.exp(scores - norm_row), 0.0)


def value_kernel(first_key, group, limit_ref, pos_ref, q_ref, g_ref, n_ref, k_ref, o_ref):
    kv = pl.program_id(0)
    total = None
    for member in range(group):
        cols = slice(member * HD, (member + 1) * HD)
        prob = prob_t(
            k_ref[...], q_ref[:, cols], n_ref[0, member : member + 1, :],
            limit_ref[kv * group + member], first_key, pos_ref[0],
        )
        part = jnp.dot(prob.astype(BF16), g_ref[:, cols], preferred_element_type=F32)
        total = part if total is None else total + part
    o_ref[...] = total.astype(o_ref.dtype)


def value_part(first_key, group, out_type, limits, pos, query, grad, norm_t, keys):
    tok_len, rows = query.shape[0], keys.shape[0]
    kv_local = keys.shape[1] // HD
    smem = pl.BlockSpec(memory_space=pltpu.SMEM)
    wide = pl.BlockSpec((tok_len, group * HD), lambda i: (0, i))
    return pl.pallas_call(
        functools.partial(value_kernel, first_key, group),
        grid=(kv_local,),
        out_shape=jax.ShapeDtypeStruct((rows, kv_local * HD), out_type),
        in_specs=[
            smem, smem, wide, wide,
            pl.BlockSpec((1, group, tok_len), lambda i: (i, 0, 0)),
            pl.BlockSpec((rows, HD), lambda i: (0, i)),
        ],
        out_specs=pl.BlockSpec((rows, HD), lambda i: (0, i)),
        cost_estimate=pl.CostEstimate(
            flops=3_000_000_000, bytes_accessed=4_000_000, transcendentals=0
        ),
        name=f"value_part_{first_key}",
    )(limits, pos, query, grad, norm_t, keys)


def score_kernel(firsts, group, limit_ref, pos_ref, q_ref, g_ref, n_ref, d_ref, *refs):
    count = len(firsts)
    k_refs, v_refs = refs[:count], refs[count : 2 * count]
    dq_ref, dk_refs = refs[2 * count], refs[2 * count + 1 :]
    kv = pl.program_id(0)
    queries = [None] * group
    for piece, first_key in enumerate(firsts):
        keys, values = k_refs[piece][...], v_refs[piece][...]
        key_total = None
        for member in range(group):
            cols = slice(member * HD, (member + 1) * HD)
            query = q_ref[:, cols]
            prob = prob_t(
                keys, query, n_ref[0, member : member + 1, :],
                limit_ref[kv * group + member], first_key, pos_ref[0],
            )
            dprob = lax.dot_general(
                values, g_ref[:, cols], (((1,), (1,)), ((), ())), preferred_element_type=F32
            )
            dscore = (
                QUERY_SCALE * prob * (dprob - d_ref[0, member : member + 1, :])
            ).astype(BF16)
            part = jnp.dot(dscore, query, preferred_element_type=F32)
            key_total = part if key_total is None else key_total + part
            part = lax.dot_general(
                dscore, keys, (((0,), (0,)), ((), ())), preferred_element_type=F32
            )
            queries[member] = part if queries[member] is None else queries[member] + part
        dk_refs[piece][...] = key_total.astype(dk_refs[piece].dtype)
    for member in range(group):
        dq_ref[:, member * HD : (member + 1) * HD] = queries[member].astype(dq_ref.dtype)


def score_part(firsts, group, types, limits, pos, query, grad, norm_t, delta_t, keys, values):
    tok_len = query.shape[0]
    kv_local = keys[0].shape[1] // HD
    smem = pl.BlockSpec(memory_space=pltpu.SMEM)
    wide = pl.BlockSpec((tok_len, group * HD), lambda i: (0, i))
    rows_t = pl.BlockSpec((1, group, tok_len), lambda i: (i, 0, 0))
    narrow = [pl.BlockSpec((k.shape[0], HD), lambda i: (0, i)) for k in keys]
    return pl.pallas_call(
        functools.partial(score_kernel, firsts, group),
        grid=(kv_local,),
        out_shape=[jax.ShapeDtypeStruct(query.shape, BF16)]
        + [jax.ShapeDtypeStruct(k.shape, t) for k, t in zip(keys, types)],
        in_specs=[smem, smem, wide, wide, rows_t, rows_t] + narrow + narrow,
        out_specs=[wide] + narrow,
        cost_estimate=pl.CostEstimate(
            flops=20_000_000_000, bytes_accessed=8_000_000, transcendentals=0
        ),
        name="score_part",
    )(limits, pos, query, grad, norm_t, delta_t, *keys, *values)


def bit_orders(bits, streams):
    heads = [(2, 0, 1), (0, 1, 2), (1, 0, 2), (2, 1, 0)] if bits >= 3 else [tuple(range(bits))]
    orders = []
    for s in range(streams):
        head = heads[s % len(heads)]
        orders.append(tuple(head) + tuple(range(len(head), bits)))
    return orders


def weight_kernel(
    n, n_head, streams,
    a_ref, v_ref, w_ref, rs_ref, cs_ref, upd_ref, new_ref,
    acc, sbuf, rbuf, xs, xr, scaled_ref, s_sem, r_sem, xs_sem, xr_sem,
):
    bits, head_bits = int(math.log2(n)), int(math.log2(n_head))
    me, hd = lax.axis_index("tok"), lax.axis_index("head")
    width = acc.shape[-1]
    rows = acc.shape[2]
    orders = bit_orders(bits, streams)

    def bit_of(index, k):
        return lax.rem(index // (1 << k), 2)

    def flipped(index, k):
        return index + (1 << k) * (1 - 2 * bit_of(index, k))

    partners = [{"tok": flipped(me, k)} for k in range(bits)]
    partners += [{"head": flipped(hd, k)} for k in range(head_bits)]
    barrier = pltpu.get_barrier_semaphore()
    for partner in partners:
        pl.semaphore_signal(barrier, inc=1, device_id=partner, device_id_type=MESH)

    def block_at(order, phase, j, other):
        index = 0
        for k in order[:phase]:
            index = index + (1 << k) * bit_of(me, k)
        mine = bit_of(me, order[phase])
        index = index + (1 << order[phase]) * ((1 - mine) if other else mine)
        for i, k in enumerate(sorted(order[phase + 1 :])):
            index = index + (1 << k) * lax.rem(j // (1 << i), 2)
        return index

    counts = [n >> (p + 1) for p in range(bits)]
    starts = [sum(counts[:p]) for p in range(bits)]

    def copy_of(s, p):
        here = pl.ds(starts[p], counts[p])
        return pltpu.make_async_remote_copy(
            src_ref=sbuf.at[s, here],
            dst_ref=rbuf.at[s, here],
            send_sem=s_sem.at[s, p],
            recv_sem=r_sem.at[s, p],
            device_id=partners[orders[s][p]],
            device_id_type=MESH,
        )

    def product(s, block):
        return jnp.dot(
            a_ref[block], v_ref[:, s * width : (s + 1) * width], preferred_element_type=F32
        )

    for s in range(streams):
        @pl.loop(0, counts[0])
        def _(j, s=s):
            sbuf[s, j] = product(s, block_at(orders[s], 0, j, True)).astype(BF16)

        if s == 0:
            pl.semaphore_wait(barrier, len(partners))
        copy_of(s, 0).start()
    for s in range(streams):
        @pl.loop(0, counts[0])
        def _(j, s=s):
            block = block_at(orders[s], 0, j, False)
            acc[s, block] = product(s, block)

    weight_f = w_ref[...].astype(F32)
    weight_sum = jnp.sum(weight_f * weight_f)

    for p in range(bits):
        for s in range(streams):
            copy_of(s, p).wait_recv()

            @pl.loop(0, counts[p])
            def _(j, s=s, p=p):
                block = block_at(orders[s], p, j, False)
                acc[s, block] = acc[s, block] + rbuf[s, starts[p] + j].astype(F32)

            if p + 1 < bits:
                @pl.loop(0, counts[p + 1])
                def _(j, s=s, p=p):
                    block = block_at(orders[s], p + 1, j, True)
                    sbuf[s, starts[p + 1] + j] = acc[s, block].astype(BF16)

                copy_of(s, p + 1).start()

    total_width = width * streams
    row_sum = jnp.zeros((rows, 1), F32)
    for s in range(streams):
        wg = acc[s, me]
        row_sum = row_sum + jnp.sum(wg * wg, axis=1, keepdims=True)
    row_mix = DECAY_RATE * rs_ref[...] + (1.0 - DECAY_RATE) * (row_sum / total_width)
    row_mean = jnp.sum(row_mix) / rows
    scaled_sum = jnp.float32(0.0)
    for s in range(streams):
        wg = acc[s, me]
        cols = slice(s * width, (s + 1) * width)
        col_new = jnp.sum(wg * wg, axis=0, keepdims=True) / rows
        col_mix = DECAY_RATE * cs_ref[:, cols] + (1.0 - DECAY_RATE) * col_new
        scaled = wg / jnp.sqrt(row_mix * col_mix / row_mean)
        scaled_ref[:, cols] = scaled
        scaled_sum = scaled_sum + jnp.sum(scaled * scaled)

    xs[0, :8] = jnp.full((8, 128), scaled_sum, F32)
    xs[0, 8:] = jnp.full((8, 128), weight_sum, F32)
    for i, partner in enumerate(partners):
        copy = pltpu.make_async_remote_copy(
            src_ref=xs.at[i], dst_ref=xr.at[i],
            send_sem=xs_sem.at[i], recv_sem=xr_sem.at[i],
            device_id=partner, device_id_type=MESH,
        )
        copy.start()
        copy.wait()
        xs[i + 1] = xs[i] + xr[i]
    sums = xs[len(partners)]
    size = float(rows * n * total_width * n_head)
    rms_scaled = jnp.sqrt(sums[0:1, 0:1] / size)
    rms_weight = jnp.sqrt(sums[8:9, 0:1] / size)
    update = rms_weight * scaled_ref[...] / jnp.maximum(1.0, rms_scaled)
    upd_ref[...] = update
    new_ref[...] = (w_ref[...].astype(F32) - LEARN_RATE * update).astype(BF16)
    for p in range(bits):
        for s in range(streams):
            copy_of(s, p).wait_send()


def weight_update(n, n_head, act_t, value_grad, weight, row_state, col_state):
    rows, width = act_t.shape[1], value_grad.shape[1]
    streams = 4 if width % 512 == 0 else 1
    part = width // streams
    bits, head_bits = int(math.log2(n)), int(math.log2(n_head))
    steps = bits + head_bits
    vmem = pl.BlockSpec(memory_space=pltpu.VMEM)
    return pl.pallas_call(
        functools.partial(weight_kernel, n, n_head, streams),
        out_shape=[
            jax.ShapeDtypeStruct((rows, width), F32),
            jax.ShapeDtypeStruct((rows, width), BF16),
        ],
        in_specs=[vmem] * 5,
        out_specs=[vmem] * 2,
        scratch_shapes=[
            pltpu.VMEM((streams, n, rows, part), F32),
            pltpu.VMEM((streams, n - 1, rows, part), BF16),
            pltpu.VMEM((streams, n - 1, rows, part), BF16),
            pltpu.VMEM((steps + 1, 16, 128), F32),
            pltpu.VMEM((steps, 16, 128), F32),
            pltpu.VMEM((rows, width), F32),
            pltpu.SemaphoreType.DMA((streams, bits)),
            pltpu.SemaphoreType.DMA((streams, bits)),
            pltpu.SemaphoreType.DMA((steps,)),
            pltpu.SemaphoreType.DMA((steps,)),
        ],
        compiler_params=pltpu.CompilerParams(
            collective_id=0, has_side_effects=True, vmem_limit_bytes=56 * 1024 * 1024
        ),
        cost_estimate=pl.CostEstimate(
            flops=60_000_000_000, bytes_accessed=8_000_000, transcendentals=0
        ),
        name="weight_update",
    )(act_t, value_grad, weight, row_state, col_state)


def shards(
    query_rows, key_rows, value_rows, out_grad, log_norm, delta_rows, window_len,
    activations, value_weight, row_state, col_state, *, n, n_head,
):
    tok_len = query_rows.shape[0]
    kv_local = key_rows.shape[1] // HD
    group = query_rows.shape[1] // key_rows.shape[1]
    reach = (WINDOW + tok_len - 1) // tok_len
    offsets = list(range(1, reach + 1))
    pos = (lax.axis_index("tok") * tok_len).astype(jnp.int32).reshape(1)
    norm_t = log_norm.T.reshape(kv_local, group, tok_len)
    delta_t = delta_rows.T.reshape(kv_local, group, tok_len)
    act_t = activations.T.reshape(n, activations.shape[1] // n, tok_len)

    def sent_rows(offset):
        return min(tok_len, WINDOW - (offset - 1) * tok_len)

    def first_of(offset):
        return max(0, WINDOW - offset * tok_len)

    far_keys = [passed_along(key_rows[tok_len - sent_rows(o) :], "tok", o) for o in offsets]

    def value_of(first_key, out_type, keys):
        return value_part(
            first_key, group, out_type, window_len, pos, query_rows, out_grad, norm_t, keys
        )

    def gathered(own, far):
        total = own
        for o, piece in zip(offsets, far):
            arrived = passed_along(piece, "tok", -o).astype(F32)
            total = total + jnp.pad(arrived, ((tok_len - arrived.shape[0], 0), (0, 0)))
        return total.astype(BF16)

    value_own = value_of(WINDOW, F32, key_rows)
    late_values, value_own = lax.optimization_barrier((value_rows, value_own))
    far_values = [passed_along(late_values[tok_len - sent_rows(o) :], "tok", o) for o in offsets]
    value_far = [value_of(first_of(o), BF16, k) for o, k in zip(offsets, far_keys)]
    value_grad = gathered(value_own, value_far)
    firsts = tuple([WINDOW] + [first_of(o) for o in offsets])
    query_grad, key_own, *key_far = score_part(
        firsts, group, [F32] + [BF16] * reach, window_len, pos, query_rows, out_grad,
        norm_t, delta_t, [key_rows] + far_keys, [value_rows] + far_values,
    )
    key_grad = gathered(key_own, key_far)
    update_dir, new_weight = weight_update(
        n, n_head, act_t, value_grad, value_weight, row_state.reshape(-1, 1), col_state
    )
    return (query_grad, key_grad, value_grad, new_weight, update_dir)


def solution(mesh):
    both = P("tok", "head")
    return jax.shard_map(
        functools.partial(shards, n=mesh.shape["tok"], n_head=mesh.shape["head"]),
        mesh=mesh,
        in_specs=(
            both, both, both, both, both, both, P("head"), P("tok", None),
            both, P("head", "tok"), both,
        ),
        out_specs=(both,) * 5,
        check_vma=False,
    )
```
